256 devices in a mesh: hi: 8 (over y, core), lo: 32 (over z, x).
Axes of the slice: x: 4, y: 4, z: 8, core: 2. Of those that a mesh axis runs over, the one named last changes fastest.
Arguments:
- grm: bfloat16 [8, 32, 64, 8, 2048], P(None, 'lo', None, 'hi'), as said below
- right_sides: float32 [16384, 512], P(('hi', 'lo')), may hold values from -6 to 6
- inv_diag: float32 [16384], P(('hi', 'lo')), may hold values from 0.3 to 1
- bases: float32 [16384, 576], P(('hi', 'lo')), may hold values from -0.75 to 0.75
- couplings: float32 [9, 64, 64], replicated, as said below
- level_map: int32 [8], replicated, may hold values from 0 to 7, each once
- variance: float32 [2], replicated, may hold values from 0.3 to 1.5
- iters_per_column: int32 [512], replicated, may hold values from 1 to 3
Outputs:
- solution: float32 [16384, 512], P(('hi', 'lo'))
- residual: float32 [16384, 512], P(('hi', 'lo'))
The draws below stay inside these ranges and needn't reach their ends.
Inputs may be any that keep to these rules, and one draw needn't show every extreme that they name: `grm`: G is symmetric and positive definite. `couplings`: each of the 9 matrices is symmetric and positive definite. `level_map`: a permutation of the levels.
All inputs are finite; a program needn't handle non-finite values.
Results may differ from the reference program's by a relative error of at most 0.0055.
Values may be sent and summed in bfloat16 or wider, within the bound.
A program may use at most 64 MiB of HBM per device.

```python
import math
import jax
import jax.numpy as jnp
from jax import lax

ROWS_DEV = 64
RHS = 512
RANK = 64
LEVELS = 8
ITERS = 3
HI_BLOCKS = 8
LO_BLOCKS = 32
SAMPLES = 16384
N_HI = 8
N_LO = 32


def draw_grm(key, part):
    entries = jax.random.normal(key, (SAMPLES, SAMPLES), jnp.float32)
    spread = 0.45 / math.sqrt(2.0 * SAMPLES)
    symmetric = (entries + entries.T) * spread + jnp.eye(SAMPLES, dtype=jnp.float32)
    return symmetric.astype(jnp.bfloat16).reshape(HI_BLOCKS, LO_BLOCKS, ROWS_DEV, HI_BLOCKS, LO_BLOCKS * ROWS_DEV)


def draw_couplings(key, part):
    factors = jax.random.normal(jax.random.fold_in(key, 11), (LEVELS + 1, RANK, RANK), jnp.float32)
    low_end = math.log(0.3)
    high_end = math.log(1.0)
    level_scale = jnp.exp(jax.random.uniform(jax.random.fold_in(key, 12), (LEVELS + 1,), jnp.float32, low_end, high_end))
    gram = jnp.einsum('lij,lkj->lik', factors, factors, precision=lax.Precision.HIGHEST) / RANK
    gram = gram + 0.25 * jnp.eye(RANK, dtype=jnp.float32)[None]
    return gram * level_scale[:, None, None]


def place_ends(result, rng, least, high):
    index_at = [jax.random.randint(jax.random.fold_in(rng, axis), (), 0, length) for axis, length in enumerate(result.shape)]
    widest = result.shape.index(max(result.shape))
    beside = index_at[:widest] + [(index_at[widest] + 1) % result.shape[widest]] + index_at[widest + 1:]
    return result.at[tuple(index_at)].set(least).at[tuple(beside)].set(high)


def block_scale(key, dims, cuts, smallest, top_value):
    level, own = 1.0, jax.random.fold_in(key, 6)
    for position, shards_of in cuts:
        steps = jnp.exp(jax.random.uniform(jax.random.fold_in(own, position), (shards_of,), jnp.float32, smallest / len(cuts), top_value / len(cuts)))
        level = level * jnp.repeat(steps, dims[position] // shards_of).reshape([-1 if axis == position else 1 for axis in range(len(dims))])
    return level


def noise(stream_key, dims, scale, most, cuts=(), held_as=jnp.bfloat16):
    gain = block_scale(stream_key, dims, cuts, -0.22, 0.18) if cuts else 1.0
    values = jax.random.normal(stream_key, dims, jnp.float32) * scale * gain
    return jnp.minimum(jnp.maximum(values, -most), most).astype(held_as)


def setup_inputs(seed: int = 0) -> dict:
    key_of = jax.random.split(jax.random.key(seed), 9)
    return {
        "grm": draw_grm(jax.random.fold_in(key_of[8], 71), 0),
        "right_sides": noise(key_of[1], (SAMPLES, RHS), 1.0, 6.0, ((0, 256),), jnp.float32),
        "inv_diag": jnp.clip(jnp.exp(math.log(1.0) - 1.2039728 * jax.random.uniform(key_of[2], (SAMPLES,), jnp.float32) ** block_scale(key_of[2], (SAMPLES,), ((0, 256),), -0.2, 0.2)), 0.3, 1.0),
        "bases": noise(key_of[3], (SAMPLES, (LEVELS + 1) * RANK), ROWS_DEV ** -0.5, 0.75, ((0, 256),), jnp.float32),
        "couplings": draw_couplings(jax.random.fold_in(key_of[8], 71), 0),
        "level_map": jax.random.permutation(key_of[5], LEVELS).astype(jnp.int32),
        "variance": jnp.clip(jnp.exp(jax.random.uniform(key_of[6], (2,), jnp.float32, math.log(0.3), math.log(1.5))), 0.3, 1.5),
        "iters_per_column": place_ends(jax.random.randint(key_of[7], (RHS,), 1, ITERS + 1), jax.random.fold_in(key_of[7], 1), 1, ITERS).astype(jnp.int32),
    }


def apply_system(grm, direction, variance):
    matrix = grm.reshape(SAMPLES, SAMPLES)
    product = jnp.dot(matrix, direction.astype(jnp.bfloat16), preferred_element_type=jnp.float32)
    return variance[0] * product + variance[1] * direction


def precondition(resid, inv_diag, bases, couplings, level_map):
    blocks = N_HI * N_LO
    bit_count = blocks.bit_length() - 1
    level_total = LEVELS + 1
    resid_blocks = resid.reshape(blocks, ROWS_DEV, RHS)
    basis_blocks = bases.reshape(blocks, ROWS_DEV, level_total * RANK)
    coefficients = jnp.einsum("dnk,dnb->dkb", basis_blocks, resid_blocks, precision=lax.Precision.HIGHEST)
    coefficients = coefficients.reshape(blocks, level_total, RANK, RHS)
    stacked = jnp.zeros_like(coefficients)
    order = jnp.arange(blocks, dtype=jnp.int32)
    level_ids = jnp.arange(level_total, dtype=jnp.int32)
    for bit_index in range(bit_count):
        level = level_map[bit_index]
        partner = jnp.bitwise_xor(order, 1 << bit_index).astype(jnp.int32)
        chosen = jnp.take(coefficients, level, axis=1)
        summed = chosen + jnp.take(chosen, partner, axis=0)
        matrix = jnp.take(couplings, level, axis=0)
        term = jnp.einsum("rs,dsb->drb", matrix, summed, precision=lax.Precision.HIGHEST)
        select = (level_ids == level).astype(jnp.float32)
        stacked = stacked + select[None, :, None, None] * term[:, None]
    total = jnp.sum(coefficients[:, LEVELS], axis=0)
    coarse = jnp.dot(couplings[LEVELS], total, precision=lax.Precision.HIGHEST)
    stacked = stacked.at[:, LEVELS].add(coarse[None])
    lifted = jnp.einsum("dnk,dkb->dnb", basis_blocks, stacked.reshape(blocks, level_total * RANK, RHS), precision=lax.Precision.HIGHEST)
    return inv_diag[:, None] * resid + lifted.reshape(SAMPLES, RHS)


def reference(grm, right_sides, inv_diag, bases, couplings, level_map, variance, iters_per_column):
    solution = jnp.zeros_like(right_sides)
    residual = right_sides
    scaled = precondition(residual, inv_diag, bases, couplings, level_map)
    direction = scaled
    energy = jnp.sum(residual * scaled, axis=0)
    for step in range(ITERS):
        image = apply_system(grm, direction, variance)
        curvature = jnp.sum(direction * image, axis=0)
        alpha = energy / curvature
        stepsize = jnp.where(step < iters_per_column, alpha, jnp.zeros_like(alpha))
        solution = solution + stepsize * direction
        residual = residual - stepsize * image
        if step + 1 < ITERS:
            scaled = precondition(residual, inv_diag, bases, couplings, level_map)
            fresh = jnp.sum(residual * scaled, axis=0)
            direction = scaled + (fresh / energy) * direction
            energy = fresh
    return solution, residual
```

```python
import functools

import jax
import jax.numpy as jnp
from jax import lax
from jax.experimental import pallas as pl
from jax.experimental.pallas import tpu as pltpu
from jax.sharding import Mesh
from jax.sharding import PartitionSpec as P

ITERS = 3
LO = ("z", "x")
HI = ("y", "c")
HI_LO = ("y", "c", "z", "x")
NY, NC, NZ, NX = 4, 2, 8, 4
HIGHEST = lax.Precision.HIGHEST
F32, BF16 = jnp.float32, jnp.bfloat16

GATHER_KEYS = (
    [("az", k, 0) for k in (7, 1, 6, 2, 5, 3)]
    + [("az+", 4, 0), ("az-", 4, 0)]
    + [(kind, k, 0) for kind in ("ax+", "ax-", "af+", "af-") for k in range(8)]
    + [(kind, 0, 0) for kind in ("bx+", "bx-", "bf+", "bf-")]
    + [("bz", k, d) for k in (7, 1, 6, 2, 5, 3) for d in range(4)]
    + [(kind, 4, d) for kind in ("bz+", "bz-") for d in range(4)]
)
GATHER_ID = {key: n for n, key in enumerate(GATHER_KEYS)}
ROWS = {
    "az": (0, 32), "az+": (0, 16), "az-": (16, 16),
    "ax+": (0, 32), "ax-": (0, 32), "af+": (0, 16), "af-": (16, 16),
    "bx+": (32, 32), "bx-": (32, 32), "bf+": (32, 16), "bf-": (48, 16),
    "bz": (32, 32), "bz+": (32, 16), "bz-": (48, 16),
}


def dot(a, b, precision=HIGHEST):
    return jnp.dot(a, b, precision=precision, preferred_element_type=F32)


def kernel(
    var_ref, grm_ref, rhs_ref, diag_ref, bt_ref, bk_ref, bc_ref, kc_ref, iters_ref,
    x_ref, r_ref,
    g_ref, v_ref, vc_ref, co_ref, cb_ref, xb_ref,
    y_ref, u_ref, w_ref, p_ref, s_ref, q_ref, ul_ref, ml_ref, tu_ref, tq_ref,
    p1_ref, r1_ref, q2_ref, qb_ref, r2_ref,
    pc_ref, rc_ref, ack_ref, bck_ref,
    as_ref, ah_ref, bs_ref, bx_ref, zs_ref, bz_ref, xa_ref, ta_ref,
    row_ref,
    g_sem, ex_send, ex_recv, ag_send, ag_recv, r1_send, r1_recv, r2_send, r2_recv,
    ar_send, ar_recv, mc_send, mc_recv,
):
    y, c, z, x = (lax.axis_index(name) for name in HI_LO)
    hi = y * 2 + c

    def dev(**where):
        return where

    def hi_dev(d):
        to = (hi + d) % 8
        return {"y": to // 2, "c": to % 2}

    def remote(src, dst, send, recv, to):
        return pltpu.make_async_remote_copy(
            src_ref=src, dst_ref=dst, send_sem=send, recv_sem=recv,
            device_id=to, device_id_type=pl.DeviceIdType.MESH,
        )

    loads = []
    for k in range(NZ):
        at = pl.multiple_of((z + k) % NZ * 256, 256)
        loads.append(
            pltpu.make_async_copy(
                grm_ref.at[:, :, pl.ds(at, 256)], g_ref.at[:, :, pl.ds(k * 256, 256)], g_sem.at[k]
            )
        )
        loads[-1].start()

    barrier = pltpu.get_barrier_semaphore()
    near = [{"x": (x + d) % NX} for d in range(1, NX)]
    near += [{"z": (z + d) % NZ} for d in range(1, NZ)]
    near += [hi_dev(d) for d in range(1, 8)]
    for to in near:
        pl.semaphore_signal(barrier, inc=1, device_id=to, device_id_type=pl.DeviceIdType.MESH)
    zero = jnp.zeros((64, 512), F32)
    for ref in (u_ref, w_ref, p_ref, s_ref, q_ref, tq_ref, x_ref):
        ref[...] = zero
    r_ref[...] = rhs_ref[...]
    y_ref[...] = rhs_ref[...]
    row_ref[...] = jnp.ones_like(row_ref)
    vc_ref[0, x] = bc_ref[...]
    bck_ref[...] = dot(bc_ref[:, :64].astype(F32) + bc_ref[:, 64:].astype(F32), kc_ref[...])
    pl.semaphore_wait(barrier, len(near))

    def coarse_z(d):
        return remote(vc_ref.at[0, x], vc_ref.at[8 - d, x], mc_send.at[0], mc_recv.at[d - 1], {"z": (z + d) % NZ})

    def coarse_x(d):
        return remote(vc_ref.at[:, x], vc_ref.at[:, x], mc_send.at[1], mc_recv.at[6 + d], {"x": (x + d) % NX})

    def coarse_x_in(d):
        at = vc_ref.at[:, (x + NX - d) % NX]
        return remote(at, at, mc_send.at[1], mc_recv.at[6 + d], {"x": (x + d) % NX})

    def coarse_r(d):
        return remote(pc_ref.at[(hi + d) % 8], rc_ref.at[d - 1], mc_send.at[2], mc_recv.at[9 + d], hi_dev(d))

    for d in range(1, NZ):
        coarse_z(d).start()

    partners = [
        {"x": x + 1 - 2 * (x % 2)}, {"x": (x + 2) % 4},
        {"z": z + 1 - 2 * (z % 2)}, {"z": z + 2 - 4 * ((z // 2) % 2)}, {"z": (z + 4) % 8},
        {"c": 1 - c}, {"y": y + 1 - 2 * (y % 2)}, {"y": (y + 2) % 4},
    ]

    def exchange(i, g):
        return remote(cb_ref.at[i, g], xb_ref.at[i, g], ex_send.at[i], ex_recv.at[i, g], partners[g])

    def piece(i, kind, k, d, slot_from, slot_to, to):
        at, rows = ROWS[kind]
        return remote(
            v_ref.at[i, slot_from, pl.ds(at, rows)], v_ref.at[i, slot_to, pl.ds(at, rows)],
            ag_send.at[i], ag_recv.at[i, GATHER_ID[kind, k, d]], to,
        )

    def slot(k, d):
        return k * NX + (x + d) % NX

    up, down = {"z": (z + 1) % NZ}, {"z": (z + NZ - 1) % NZ}
    right, left = {"x": (x + 1) % NX}, {"x": (x + NX - 1) % NX}

    def along_z(i, kind, k, d):
        if k in (0, 7, 6, 5):
            to = (k - 1) % 8
            name = kind + "+" if to == 4 else kind
            piece(i, name, to, d, slot(k, d), slot(to, d), up).start()
        if k in (0, 1, 2, 3):
            to = k + 1
            name = kind + "-" if to == 4 else kind
            piece(i, name, to, d, slot(k, d), slot(to, d), down).start()

    def got(i, kind, k, d, where):
        piece(i, kind, k, d, where, where, up).wait_recv()

    def along_x(i, kind, k):
        piece(i, kind + "+", k, 0, slot(k, 0), slot(k, 0), right).start()
        piece(i, kind + "-", k, 0, slot(k, 0), slot(k, 0), left).start()

    def turn_x(i, kind, name, k):
        got(i, kind + "+", k, 0, slot(k, 3))
        piece(i, name + "+", k, 0, slot(k, 3), slot(k, 3), right).start()
        got(i, kind + "-", k, 0, slot(k, 1))
        piece(i, name + "-", k, 0, slot(k, 1), slot(k, 1), left).start()

    def far_x(i, name, k):
        got(i, name + "+", k, 0, slot(k, 2))
        got(i, name + "-", k, 0, slot(k, 2))

    def came_z(i, kind, k, d):
        if k == 4:
            got(i, kind + "+", 4, d, slot(4, d))
            got(i, kind + "-", 4, d, slot(4, d))
        else:
            got(i, kind, k, d, slot(k, d))
            along_z(i, kind, k, d)

    def gather_start(i):
        along_z(i, "az", 0, 0)
        along_x(i, "bx", 0)
        along_x(i, "ax", 0)
        along_z(i, "bz", 0, 0)

    def gather_1(i):
        for k in (7, 1):
            came_z(i, "az", k, 0)
            along_x(i, "ax", k)
        turn_x(i, "bx", "bf", 0)
        along_z(i, "bz", 0, 3)
        along_z(i, "bz", 0, 1)
        turn_x(i, "ax", "af", 0)
        for k in (7, 1):
            came_z(i, "bz", k, 0)

    def gather_2(i):
        for k in (6, 2):
            came_z(i, "az", k, 0)
            along_x(i, "ax", k)
        far_x(i, "bf", 0)
        along_z(i, "bz", 0, 2)
        for k in (7, 1):
            turn_x(i, "ax", "af", k)
        for d in (3, 1):
            for k in (7, 1):
                came_z(i, "bz", k, d)
        for k in (6, 2):
            came_z(i, "bz", k, 0)

    def gather_3(i):
        for k in (5, 3):
            came_z(i, "az", k, 0)
            along_x(i, "ax", k)
        for k in (6, 2):
            turn_x(i, "ax", "af", k)
        for k in (7, 1):
            came_z(i, "bz", k, 2)
        for d in (3, 1):
            for k in (6, 2):
                came_z(i, "bz", k, d)
        for k in (5, 3):
            came_z(i, "bz", k, 0)

    def gather_4(i):
        came_z(i, "az", 4, 0)
        along_x(i, "ax", 4)
        for k in (5, 3):
            turn_x(i, "ax", "af", k)
        for k in (6, 2):
            came_z(i, "bz", k, 2)
        for d in (3, 1):
            for k in (5, 3):
                came_z(i, "bz", k, d)
        came_z(i, "bz", 4, 0)

    def gather_5(i):
        turn_x(i, "ax", "af", 4)
        for k in (5, 3):
            came_z(i, "bz", k, 2)
        for d in (3, 1, 2):
            came_z(i, "bz", 4, d)
        for k in range(8):
            far_x(i, "af", k)

    def sum_hi(j, d):
        return remote(as_ref.at[j, (hi + d) % 8], ah_ref.at[j, d - 1], ar_send.at[j, 0], ar_recv.at[j, d - 1], hi_dev(d))

    def sum_x(j, d):
        return remote(bs_ref.at[j, (x + d) % 4], bx_ref.at[j, d - 1], ar_send.at[j, 1], ar_recv.at[j, 6 + d], {"x": (x + d) % NX})

    def sum_z(j, d):
        return remote(zs_ref.at[j], bz_ref.at[j, d - 1], ar_send.at[j, 2], ar_recv.at[j, 9 + d], {"z": (z + d) % NZ})

    def all_x(j, d):
        return remote(xa_ref.at[j, x], xa_ref.at[j, x], ar_send.at[j, 3], ar_recv.at[j, 16 + d], {"x": (x + d) % NX})

    def all_x_in(j, d):
        at = xa_ref.at[j, (x + NX - d) % NX]
        return remote(at, at, ar_send.at[j, 3], ar_recv.at[j, 16 + d], {"x": (x + d) % NX})

    def all_hi(j, d):
        return remote(ta_ref.at[j, hi], ta_ref.at[j, hi], ar_send.at[j, 4], ar_recv.at[j, 19 + d], hi_dev(d))

    def all_hi_in(j, d):
        at = ta_ref.at[j, (hi + 8 - d) % 8]
        return remote(at, at, ar_send.at[j, 4], ar_recv.at[j, 19 + d], hi_dev(d))

    def sums_start(j, total):
        gamma = jnp.sum(r_ref[...] * u_ref[...], axis=0, keepdims=True)
        delta = jnp.sum(u_ref[...] * w_ref[...], axis=0, keepdims=True)
        eta = jnp.sum(u_ref[...] * s_ref[...] + p_ref[...] * w_ref[...], axis=0, keepdims=True)
        line = lax.broadcasted_iota(jnp.int32, (8, 512), 0)
        rows = jnp.where(line == 0, gamma, jnp.where(line == 1, delta, jnp.where(line == 2, eta, 0.0)))
        for h in range(8):
            as_ref[j, h, 0:8, :] = total[h * 8 : (h + 1) * 8] if total is not None else jnp.zeros((8, 512), F32)
            as_ref[j, h, 8:16, :] = rows
        for d in range(1, 8):
            sum_hi(j, d).start()

    def sums_1(j):
        whole = as_ref[j, hi]
        for d in range(1, 8):
            sum_hi(j, d).wait_recv()
            whole = whole + ah_ref[j, d - 1]
        for k in range(4):
            bs_ref[j, k] = whole[:, k * 128 : (k + 1) * 128]
        for d in range(1, 4):
            sum_x(j, d).start()

    def sums_2(j):
        whole = bs_ref[j, x]
        for d in range(1, 4):
            sum_x(j, d).wait_recv()
            whole = whole + bx_ref[j, d - 1]
        zs_ref[j] = whole
        for d in range(1, 8):
            sum_z(j, d).start()

    def sums_3(j):
        whole = zs_ref[j]
        for d in range(1, 8):
            sum_z(j, d).wait_recv()
            whole = whole + bz_ref[j, d - 1]
        xa_ref[j, x] = whole
        for d in range(1, 4):
            all_x(j, d).start()

    def sums_4(j, coarse):
        for d in range(1, 4):
            all_x_in(j, d).wait_recv()
        if coarse:
            for k in range(4):
                ta_ref[j, hi, k] = xa_ref[j, k, 0:8, :]
            for d in range(1, 8):
                all_hi(j, d).start()

    def sums_of(j):
        return [
            jnp.concatenate([xa_ref[j, k, 8 + n : 9 + n, :] for k in range(4)], axis=1) for n in range(3)
        ]

    def sums_5(j):
        for d in range(1, 8):
            all_hi_in(j, d).wait_recv()
        return jnp.concatenate([ta_ref[j, :, k].reshape(64, 128) for k in range(4)], axis=1)

    def to_core(i):
        return remote(p1_ref.at[i], r1_ref.at[i], r1_send.at[i], r1_recv.at[i], {"c": 1 - c})

    def to_y(i, d):
        return remote(qb_ref.at[i, d - 1], r2_ref.at[i, d - 1], r2_send.at[i], r2_recv.at[i, d - 1], {"y": (y + d) % NY})

    def rows_of(core):
        return jnp.concatenate([g_ref[2 * k + core] for k in range(4)], axis=0)

    def times_grm(i):
        dense = v_ref[i].reshape(2048, 512)
        p1_ref[i] = dot(rows_of(1 - c), dense, None).astype(BF16).reshape(4, 64, 512)
        to_core(i).start()
        own = dot(rows_of(c), dense, None).reshape(4, 64, 512)
        to_core(i).wait_recv()
        q2_ref[...] = own + r1_ref[i].astype(F32)
        for d in range(1, 4):
            qb_ref[i, d - 1] = q2_ref[(y + d) % NY].astype(BF16)
            to_y(i, d).start()

    def product(i):
        for d in range(1, 4):
            to_y(i, d).wait_recv()
        whole = q2_ref[y]
        for d in range(1, 4):
            whole = whole + r2_ref[i, d - 1].astype(F32)
        return whole

    def weights(step, gamma, delta, eta):
        beta = jnp.where(step == 0, 0.0, gamma / row_ref[0:1])
        curve = delta + beta * eta + beta * beta * row_ref[1:2]
        alpha = gamma / curve
        row_ref[0:1] = gamma
        row_ref[1:2] = curve
        row_ref[2:3] = beta
        row_ref[3:4] = alpha
        return beta, alpha, jnp.where(step < iters_ref[...], alpha, 0.0)

    def body(i, carry):
        coeff = dot(bt_ref[...], y_ref[...])
        co_ref[...] = coeff[:512]
        cb_ref[i] = coeff[:512].astype(BF16).reshape(8, 64, 512)
        sums_start(i, coeff[512:])
        for g in (4, 3, 1, 7, 2, 0, 6, 5):
            exchange(i, g).start()

        @pl.when(i == 0)
        def _():
            for d in range(1, NZ):
                coarse_z(d).wait_recv()
            for d in range(1, NX):
                coarse_x(d).start()

        sums_1(i)
        sums_2(i)
        for g in (5, 6, 0, 2, 7, 1, 3, 4):
            exchange(i, g).wait_recv()
        both = co_ref[...] + xb_ref[i].astype(F32).reshape(512, 512)
        ml_ref[...] = diag_ref[:, 0:1] * y_ref[...] + dot(bk_ref[...], both)
        sums_3(i)
        sums_4(i, True)

        @pl.when(i == 0)
        def _():
            ul_ref[...] = ml_ref[...]

        @pl.when(i > 0)
        def _():
            beta, alpha, stepsize = weights(i - 1, *sums_of(i))
            q = ml_ref[...] + beta * q_ref[...]
            ul_ref[...] = ul_ref[...] - alpha * q
            q_ref[...] = q

        v_ref[i, x] = ul_ref[...].astype(BF16)
        gather_start(i)

        @pl.when(i > 0)
        def _():
            beta = row_ref[2:3]
            stepsize = jnp.where(i - 1 < iters_ref[...], row_ref[3:4], 0.0)
            p = u_ref[...] + beta * p_ref[...]
            s = w_ref[...] + beta * s_ref[...]
            x_ref[...] = x_ref[...] + stepsize * p
            r_ref[...] = r_ref[...] - stepsize * s
            p_ref[...] = p
            s_ref[...] = s

        gather_1(i)
        gather_2(i)
        gather_3(i)

        @pl.when(i == 0)
        def _():
            for d in range(1, NX):
                coarse_x_in(d).wait_recv()
            for load in loads:
                load.wait()
            part = dot(g_ref[...].reshape(512, 2048), vc_ref[...].reshape(2048, 128), None)
            pc_ref[...] = part.reshape(8, 64, 128)
            for d in range(1, 8):
                coarse_r(d).start()

        gather_4(i)
        gather_5(i)
        times_grm(i)
        coarse = sums_5(i)

        @pl.when(i == 0)
        def _():
            whole = pc_ref[hi]
            for d in range(1, 8):
                coarse_r(d).wait_recv()
                whole = whole + rc_ref[d - 1]
            own = bc_ref[:, :64].astype(F32) + bc_ref[:, 64:].astype(F32)
            ac = var_ref[0] * (whole[:, :64] + whole[:, 64:]) + var_ref[1] * own
            ack_ref[...] = dot(ac, kc_ref[...])
            tu_ref[...] = coarse

        @pl.when(i > 0)
        def _():
            tq = coarse + row_ref[2:3] * tq_ref[...]
            tu_ref[...] = tu_ref[...] - row_ref[3:4] * tq
            tq_ref[...] = tq

        u_ref[...] = ul_ref[...] + dot(bck_ref[...], tu_ref[...])
        shift = var_ref[1] * ul_ref[...] + dot(ack_ref[...], tu_ref[...])
        w = var_ref[0] * product(i) + shift
        w_ref[...] = w
        y_ref[...] = w
        return carry

    lax.fori_loop(0, ITERS, body, 0)
    sums_start(ITERS, None)
    sums_1(ITERS)
    sums_2(ITERS)
    sums_3(ITERS)
    sums_4(ITERS, False)
    beta, alpha, stepsize = weights(ITERS - 1, *sums_of(ITERS))
    x_ref[...] = x_ref[...] + stepsize * (u_ref[...] + beta * p_ref[...])
    r_ref[...] = r_ref[...] - stepsize * (w_ref[...] + beta * s_ref[...])

    def left_all(ref, sem):
        pltpu.make_async_copy(ref, ref, sem).wait()

    for i in range(ITERS):
        left_all(cb_ref.at[i], ex_send.at[i])
        left_all(v_ref.at[i, pl.ds(0, 31)], ag_send.at[i])
        left_all(p1_ref.at[i], r1_send.at[i])
        left_all(qb_ref.at[i], r2_send.at[i])
    for j in range(ITERS + 1):
        left_all(ah_ref.at[j], ar_send.at[j, 0])
        left_all(bx_ref.at[j], ar_send.at[j, 1])
        left_all(bz_ref.at[j], ar_send.at[j, 2])
        left_all(bx_ref.at[j], ar_send.at[j, 3])
        if j < ITERS:
            left_all(ta_ref.at[j, pl.ds(0, 7)], ar_send.at[j, 4])
    left_all(vc_ref.at[pl.ds(0, 7), 0], mc_send.at[0])
    left_all(vc_ref.at[:, pl.ds(0, 3)], mc_send.at[1])
    left_all(rc_ref, mc_send.at[2])


def local(grm, right_sides, inv_diag, bases, couplings, level_map, variance, iters_per_column):
    order = jnp.concatenate([level_map, jnp.full((1,), 8, jnp.int32)])
    basis = jnp.take(bases.reshape(64, 9, 64), order, axis=1)
    matrices = jnp.take(couplings, order, axis=0)
    basis_t = basis.transpose(1, 2, 0).reshape(576, 64)
    lifted = jnp.einsum("ngr,grs->ngs", basis[:, :8], matrices[:8], precision=HIGHEST).reshape(64, 512)
    coarse = bases[:, 512:]
    coarse_hi = coarse.astype(BF16)
    coarse_lo = (coarse - coarse_hi.astype(F32)).astype(BF16)
    vmem = pl.BlockSpec(memory_space=pltpu.VMEM)
    n = ITERS
    state = pltpu.VMEM((64, 512), F32)
    dma = pltpu.SemaphoreType.DMA
    return pl.pallas_call(
        kernel,
        name="solve",
        out_shape=(jax.ShapeDtypeStruct((64, 512), F32),) * 2,
        in_specs=[pl.BlockSpec(memory_space=pltpu.SMEM), pl.BlockSpec(memory_space=pltpu.HBM)] + [vmem] * 7,
        out_specs=(vmem, vmem),
        scratch_shapes=[
            pltpu.VMEM((8, 64, 2048), BF16),
            pltpu.VMEM((n, 32, 64, 512), BF16),
            pltpu.VMEM((8, 4, 64, 128), BF16),
            pltpu.VMEM((512, 512), F32),
            pltpu.VMEM((n, 8, 64, 512), BF16),
            pltpu.VMEM((n, 8, 64, 512), BF16),
            *[state] * 10,
            pltpu.VMEM((n, 4, 64, 512), BF16),
            pltpu.VMEM((n, 4, 64, 512), BF16),
            pltpu.VMEM((4, 64, 512), F32),
            pltpu.VMEM((n, 3, 64, 512), BF16),
            pltpu.VMEM((n, 3, 64, 512), BF16),
            pltpu.VMEM((8, 64, 128), F32),
            pltpu.VMEM((7, 64, 128), F32),
            pltpu.VMEM((64, 64), F32),
            pltpu.VMEM((64, 64), F32),
            pltpu.VMEM((n + 1, 8, 16, 512), F32),
            pltpu.VMEM((n + 1, 7, 16, 512), F32),
            pltpu.VMEM((n + 1, 4, 16, 128), F32),
            pltpu.VMEM((n + 1, 3, 16, 128), F32),
            pltpu.VMEM((n + 1, 16, 128), F32),
            pltpu.VMEM((n + 1, 7, 16, 128), F32),
            pltpu.VMEM((n + 1, 4, 16, 128), F32),
            pltpu.VMEM((n + 1, 8, 4, 8, 128), F32),
            pltpu.VMEM((8, 512), F32),
            dma((8,)),
            dma((n,)), dma((n, 8)),
            dma((n,)), dma((n, len(GATHER_KEYS))),
            dma((n,)), dma((n,)),
            dma((n,)), dma((n, 3)),
            dma((n + 1, 5)), dma((n + 1, 27)),
            dma((3,)), dma((17,)),
        ],
        compiler_params=pltpu.CompilerParams(
            collective_id=0, has_side_effects=True, vmem_limit_bytes=60 * 1024 * 1024
        ),
    )(
        variance,
        grm.reshape(8, 64, 2048),
        right_sides,
        jnp.broadcast_to(inv_diag[:, None], (64, 128)),
        basis_t,
        lifted,
        jnp.concatenate([coarse_hi, coarse_lo], axis=1),
        couplings[8],
        iters_per_column.reshape(1, 512),
    )


def solution(mesh):
    split = Mesh(mesh.devices.reshape(NY, NC, NZ, NX), HI_LO)
    return jax.shard_map(
        local,
        mesh=split,
        in_specs=(
            P(None, LO, None, HI, None),
            P(HI_LO, None),
            P(HI_LO),
            P(HI_LO, None),
            P(),
            P(),
            P(),
            P(),
        ),
        out_specs=(P(HI_LO, None), P(HI_LO, None)),
        check_vma=False,
    )
```
